32 devices in a mesh: dp: 1, tp: 32 (over x, y, z, core).
Axes of the slice: x: 2, y: 2, z: 4, core: 2. Of those that a mesh axis runs over, the one named last changes fastest.
Arguments:
- x: bfloat16 [128, 12288], P('dp')
- w_gate: bfloat16 [12288, 28672], P(None, 'tp')
- w_up: bfloat16 [12288, 28672], P(None, 'tp')
- w_down: bfloat16 [28672, 12288], P('tp')
Outputs:
- output: bfloat16 [128, 12288], P('dp')
All inputs are finite; a program needn't handle non-finite values.
Results may differ from the reference program's by a relative error of at most 0.016.
Values are sent between devices in bfloat16 or wider.
A program may use at most 2 GiB of HBM per device.

```python
import jax
import jax.numpy as jnp

ROWS = 128
D = 12288
FF = 28672


def setup_inputs(seed: int = 0, part: int = 0) -> dict:
    kx, kg, ku, kd = jax.random.split(jax.random.key(seed), 4)
    drawn = {
        "x": jax.random.normal(jax.random.fold_in(kx, part), (ROWS, D), jnp.float32),
        "w_gate": jax.random.normal(kg, (D, FF), jnp.float32) * D**-0.5,
        "w_up": jax.random.normal(ku, (D, FF), jnp.float32) * D**-0.5,
        "w_down": jax.random.normal(kd, (FF, D), jnp.float32) * FF**-0.5,
    }
    return {k: v.astype(jnp.bfloat16) for k, v in drawn.items()}


def reference(x, w_gate, w_up, w_down):
    gate = jnp.dot(x, w_gate, preferred_element_type=jnp.float32)
    up = jnp.dot(x, w_up, preferred_element_type=jnp.float32)
    hidden = (jax.nn.silu(gate) * up).astype(jnp.bfloat16)
    return jnp.dot(hidden, w_down, preferred_element_type=jnp.float32).astype(jnp.bfloat16)
```

```python
import functools

import jax
import jax.numpy as jnp
from jax import lax
from jax.experimental import pallas as pl
from jax.experimental.pallas import tpu as pltpu
from jax.sharding import PartitionSpec as P

ROWS, D, FF = 128, 12288, 896
BLK = 8
NB = ROWS // BLK
R = 512
STEPS = D // R
NS = 8
K = 4
HALF = D // 2
W = HALF // K
WH = W // 2
S = 2 * K
F32, BF16 = jnp.float32, jnp.bfloat16
MESH = pl.DeviceIdType.MESH


def kernel(
    x_hbm, wg_hbm, wu_hbm, wd_hbm, y_hbm,
    wbuf, xbuf, acc, hid, wd, own, d_send, d_recv, s1, r1, s2, r2, s3, r3, yv,
    psem, wsem, osem,
    d_ss, d_rs, s1_ss, s1_rs, s2_ss, s2_rs, s3_ss, s3_rs,
    g3_ss, g3_rs, g2_ss, g2_rs, g1_ss, g1_rs, h_ss, h_rs,
):
    me = lax.axis_index("tp")
    core = lax.rem(me, 2)
    z = lax.rem(lax.div(me, 2), 4)
    y = lax.rem(lax.div(me, 8), 2)
    x = lax.div(me, 16)
    partner = me + 1 - 2 * core
    nbr = (me + 16 * (1 - 2 * x), me + 8 * (1 - 2 * y))
    zpos = [lax.rem(z + j, 4) for j in (1, 2, 3)]
    zpeer = [me + 2 * (q - z) for q in zpos]
    coord = (x, y)

    barrier = pltpu.get_barrier_semaphore()
    for peer in (partner, *nbr, *zpeer):
        pl.semaphore_signal(barrier, inc=1, device_id={"tp": peer}, device_id_type=MESH)

    def stream(step, slot):
        rows = pl.ds(pl.multiple_of(step * R, R), R)
        return (
            pltpu.make_async_copy(wg_hbm.at[rows, :], wbuf.at[slot, :, pl.ds(0, FF)], psem.at[0, slot]),
            pltpu.make_async_copy(wu_hbm.at[rows, :], wbuf.at[slot, :, pl.ds(FF, FF)], psem.at[1, slot]),
            pltpu.make_async_copy(x_hbm.at[:, rows], xbuf.at[slot], psem.at[2, slot]),
        )

    def down(t):
        odd = lax.rem(t, 2)
        half = odd * core + (1 - odd) * (1 - core)
        cols = pl.ds(pl.multiple_of(half * HALF + lax.div(t, 2) * W, W), W)
        return pltpu.make_async_copy(wd_hbm.at[:, cols], wd.at[t], wsem.at[t])

    def project(step):
        slot = lax.rem(step, NS)
        for c in stream(step, slot):
            c.wait()
        acc[...] += jnp.dot(xbuf[slot], wbuf[slot], preferred_element_type=F32)
        return slot

    for i in range(NS):
        for c in stream(i, i):
            c.start()
    acc[...] = jnp.zeros_like(acc)

    @pl.loop(0, STEPS - NS)
    def _(step):
        slot = project(step)
        for c in stream(step + NS, slot):
            c.start()

    @pl.loop(STEPS - NS, STEPS)
    def _(step):
        down(step - (STEPS - NS)).start()
        project(step)

    gate, up = acc[:, :FF], acc[:, FF:]
    hid[...] = (jax.nn.silu(gate) * up).astype(BF16)
    pl.semaphore_wait(barrier, 6)

    def remote(src, dst, ss, rs, peer):
        return pltpu.make_async_remote_copy(
            src_ref=src, dst_ref=dst, send_sem=ss, recv_sem=rs, device_id={"tp": peer}, device_id_type=MESH
        )

    def ab(s):
        i = s % 2
        return coord[i], coord[1 - i], nbr[i], nbr[1 - i]

    def mine(s):
        return core * S + s

    def d_copy(s):
        return remote(d_send.at[s], d_recv.at[s], d_ss.at[s], d_rs.at[s], partner)

    def s1_copy(s):
        return remote(s1.at[s], r1.at[s], s1_ss.at[s], s1_rs.at[s], ab(s)[2])

    def s2_copy(s):
        return remote(s2.at[s], r2.at[s], s2_ss.at[s], s2_rs.at[s], ab(s)[3])

    def s3_copy(s, j):
        return remote(s3.at[s, j], r3.at[s, j], s3_ss.at[s, j], s3_rs.at[s, j], zpeer[j])

    def g3_copy(s, j):
        a, b, _, _ = ab(s)
        ref = yv.at[mine(s), 8 * a + 4 * b + z]
        return remote(ref, ref, g3_ss.at[s, j], g3_rs.at[s, j], zpeer[j])

    def g2_copy(s):
        a, b, _, peer = ab(s)
        ref = yv.at[mine(s), pl.ds(8 * a + 4 * b, 4)]
        return remote(ref, ref, g2_ss.at[s], g2_rs.at[s], peer)

    def g1_copy(s):
        a, _, peer, _ = ab(s)
        ref = yv.at[mine(s), pl.ds(8 * a, 8)]
        return remote(ref, ref, g1_ss.at[s], g1_rs.at[s], peer)

    def h_copy(s, i):
        a = ab(s)[0]
        ref = yv.at[mine(s), pl.ds(8 * a if i == 0 else 8 * (1 - a), 8)]
        return remote(ref, ref, h_ss.at[s, i], h_rs.at[s, i], partner)

    def out_copy(g, i):
        return pltpu.make_async_copy(yv.at[g], y_hbm.at[:, :, pl.ds(pl.multiple_of(g * WH, WH), WH)], osem.at[i])

    def subs(k):
        return (2 * k, 2 * k + 1)

    def compute(k):
        for t in (2 * k, 2 * k + 1):
            down(t).wait()
            for i, s in enumerate(subs(k)):
                p = jnp.dot(hid[...], wd[t, :, i * WH : (i + 1) * WH], preferred_element_type=F32)
                p = p.reshape(NB, BLK, WH)
                if t % 2 == 0:
                    d_send[s] = p.astype(BF16)
                    d_copy(s).start()
                else:
                    own[s] = p

    def first(k):
        for s in subs(k):
            a = ab(s)[0]
            d_copy(s).wait_recv()
            go, keep = pl.ds(8 * (1 - a), 8), pl.ds(8 * a, 8)
            s1[s] = (own[s, go] + d_recv[s, go].astype(F32)).astype(BF16)
            s1_copy(s).start()
            own[s, keep] += d_recv[s, keep].astype(F32)

    def second(k):
        for s in subs(k):
            a, b, _, _ = ab(s)
            s1_copy(s).wait_recv()
            go, keep = 4 * (1 - b), 4 * b
            s2[s] = (own[s, pl.ds(8 * a + go, 4)] + r1[s, pl.ds(go, 4)].astype(F32)).astype(BF16)
            s2_copy(s).start()
            own[s, pl.ds(8 * a + keep, 4)] += r1[s, pl.ds(keep, 4)].astype(F32)

    def third(k):
        for s in subs(k):
            a, b, _, _ = ab(s)
            s2_copy(s).wait_recv()
            base = 8 * a + 4 * b
            for j in range(3):
                q = zpos[j]
                s3[s, j] = (own[s, base + q] + r2[s, q].astype(F32)).astype(BF16)
                s3_copy(s, j).start()

    def final(k):
        for s in subs(k):
            a, b, _, _ = ab(s)
            base = 8 * a + 4 * b
            total = own[s, base + z] + r2[s, z].astype(F32)
            for j in range(3):
                s3_copy(s, j).wait_recv()
                total += r3[s, j].astype(F32)
            yv[mine(s), base + z] = total.astype(BF16)
            for j in range(3):
                g3_copy(s, j).start()

    def gather_b(k):
        for s in subs(k):
            for j in range(3):
                g3_copy(s, j).wait_recv()
            g2_copy(s).start()

    def gather_a(k):
        for s in subs(k):
            g2_copy(s).wait_recv()
            g1_copy(s).start()
            h_copy(s, 0).start()

    def gather_core(k):
        for s in subs(k):
            g1_copy(s).wait_recv()
            h_copy(s, 1).start()
            out_copy(mine(s), s).start()

    def finish(k):
        for s in subs(k):
            h_copy(s, 0).wait_recv()
            h_copy(s, 1).wait_recv()
            out_copy((1 - core) * S + s, S + s).start()

    stages = (compute, first, second, third, final, gather_b, gather_a, gather_core, finish)
    for time in range(K + len(stages) - 1):
        for i, stage in enumerate(stages):
            if 0 <= time - i < K:
                stage(time - i)

    for s in range(S):
        d_copy(s).wait_send()
        s1_copy(s).wait_send()
        s2_copy(s).wait_send()
        g2_copy(s).wait_send()
        g1_copy(s).wait_send()
        for j in range(3):
            s3_copy(s, j).wait_send()
            g3_copy(s, j).wait_send()
        for i in range(2):
            h_copy(s, i).wait_send()
        out_copy(mine(s), s).wait()
        out_copy((1 - core) * S + s, S + s).wait()


def block(x, w_gate, w_up, w_down):
    dma = pltpu.SemaphoreType.DMA
    out = pl.pallas_call(
        kernel,
        name="mlp",
        out_shape=jax.ShapeDtypeStruct((NB, BLK, D), BF16),
        in_specs=[pl.BlockSpec(memory_space=pl.ANY)] * 4,
        out_specs=pl.BlockSpec(memory_space=pl.ANY),
        scratch_shapes=[
            pltpu.VMEM((NS, R, 2 * FF), BF16),
            pltpu.VMEM((NS, ROWS, R), BF16),
            pltpu.VMEM((ROWS, 2 * FF), F32),
            pltpu.VMEM((ROWS, FF), BF16),
            pltpu.VMEM((2 * K, FF, W), BF16),
            pltpu.VMEM((S, NB, BLK, WH), F32),
            pltpu.VMEM((S, NB, BLK, WH), BF16),
            pltpu.VMEM((S, NB, BLK, WH), BF16),
            pltpu.VMEM((S, 8, BLK, WH), BF16),
            pltpu.VMEM((S, 8, BLK, WH), BF16),
            pltpu.VMEM((S, 4, BLK, WH), BF16),
            pltpu.VMEM((S, 4, BLK, WH), BF16),
            pltpu.VMEM((S, 3, BLK, WH), BF16),
            pltpu.VMEM((S, 3, BLK, WH), BF16),
            pltpu.VMEM((2 * S, NB, BLK, WH), BF16),
            dma((3, NS)),
            dma((2 * K,)),
            dma((2 * S,)),
            *[dma((S,))] * 6,
            *[dma((S, 3))] * 4,
            *[dma((S,))] * 4,
            *[dma((S, 2))] * 2,
        ],
        compiler_params=pltpu.CompilerParams(
            collective_id=0, has_side_effects=True, vmem_limit_bytes=63 * 1024 * 1024
        ),
        cost_estimate=pl.CostEstimate(flops=6 * ROWS * D * FF, bytes_accessed=6 * D * FF, transcendentals=ROWS * FF),
    )(x, w_gate, w_up, w_down)
    return out.reshape(ROWS, D)


def solution(mesh):
    return jax.shard_map(
        block,
        mesh=mesh,
        in_specs=(P("dp", None), P(None, "tp"), P(None, "tp"), P("tp", None)),
        out_specs=P("dp", None),
        check_vma=False,
    )
```

```python
import jax
import jax.numpy as jnp
from jax import lax
from jax.experimental import pallas as pl
from jax.experimental.pallas import tpu as pltpu
from jax.sharding import PartitionSpec as P

ROWS, D, FF = 128, 12288, 896
BLK = 8
NB = ROWS // BLK
R = 512
STEPS = D // R
NS = 8
HALF = D // 2
T = 512
TILES = 2 * HALF // T
PER = TILES // NS
CHUNKS = (
    (1024, "nfyx"), (512, "xyq"), (512, "yxq"), (512, "nfxy"), (512, "xyq"), (512, "yxq"), (768, "yxq"),
    (512, "nfyx"), (768, "xyq"), (512, "yxq"),
)
ORDER = (
    0, 1, 2, 3, 0, 4, 1, 5, 2, 3, 6, 4, 7, 5, 8, 6, 9, 1, 7, 2, 0, 8, 4, 9, 5, 3, 2, 7, 6, 1, 8, 4, 0, 5, 3, 9, 6,
    7, 2, 8, 3, 0, 1, 9, 4, 7, 5, 3, 0, 6, 7, 2, 3, 8, 0, 1, 7, 9, 2, 3, 4, 0, 5, 1, 7, 6, 8, 2, 5, 3, 9, 4, 2, 1,
    0, 7, 8, 6, 1, 9, 3, 5, 4, 3, 5, 4, 0, 6, 8, 0, 7, 6, 9, 8, 7, 9,
)
S = len(CHUNKS)
STARTS = [sum(w for w, _ in CHUNKS[:s]) for s in range(S)]
F32, BF16 = jnp.float32, jnp.bfloat16
MESH = pl.DeviceIdType.MESH


def kernel(
    x_hbm, wg_hbm, wu_hbm, wd_hbm, out,
    wbuf, xbuf, acc, hid, wd, own, sbuf, rbuf,
    psem, wsem, send_sem, recv_sem, send_core, recv_core,
):
    me = lax.axis_index("tp")
    core = lax.rem(me, 2)
    z = lax.rem(lax.div(me, 2), 4)
    y = lax.rem(lax.div(me, 8), 2)
    x = lax.div(me, 16)
    near, far = lax.rem(z, 2), lax.div(z, 2)
    partner = me + 1 - 2 * core
    step_n, step_f = 2 * (1 - 2 * near), 4 * (1 - 2 * far)
    bit = {"x": x, "y": y, "n": near, "f": far}
    peer = {"x": me + 16 * (1 - 2 * x), "y": me + 8 * (1 - 2 * y), "n": me + step_n, "f": me + step_f}
    flip_n, flip_f = 1 - near, 1 - far
    others = (
        (2 * far + flip_n, me + step_n),
        (2 * flip_f + near, me + step_f),
        (2 * flip_f + flip_n, me + step_n + step_f),
    )

    barrier = pltpu.get_barrier_semaphore()
    for device in (partner, peer["x"], peer["y"], *[device for _, device in others]):
        pl.semaphore_signal(barrier, inc=1, device_id={"tp": device}, device_id_type=MESH)

    def stream(step, slot):
        rows = pl.ds(pl.multiple_of(step * R, R), R)
        return (
            pltpu.make_async_copy(wg_hbm.at[rows, :], wbuf.at[slot, :, pl.ds(0, FF)], psem.at[0, slot]),
            pltpu.make_async_copy(wu_hbm.at[rows, :], wbuf.at[slot, :, pl.ds(FF, FF)], psem.at[1, slot]),
            pltpu.make_async_copy(x_hbm.at[:, rows], xbuf.at[slot], psem.at[2, slot]),
        )

    def down(t):
        odd = lax.rem(t, 2)
        half = odd * core + (1 - odd) * (1 - core)
        inner = lax.div(t, 2) * T
        src = wd_hbm.at[:, pl.ds(pl.multiple_of(half * HALF + inner, T), T)]
        return pltpu.make_async_copy(src, wd.at[odd, :, pl.ds(pl.multiple_of(inner, T), T)], wsem.at[t])

    def project(step):
        slot = lax.rem(step, NS)
        for c in stream(step, slot):
            c.wait()
        acc[...] += jnp.dot(xbuf[slot], wbuf[slot], preferred_element_type=F32)
        return slot

    for i in range(NS):
        for c in stream(i, i):
            c.start()
    acc[...] = jnp.zeros_like(acc)

    @pl.loop(0, STEPS - NS)
    def _(step):
        slot = project(step)
        for c in stream(step + NS, slot):
            c.start()

    @pl.loop(STEPS - NS, STEPS)
    def _(step):
        for i in range(PER):
            down(PER * (step - (STEPS - NS)) + i).start()
        project(step)

    gate, up = acc[:, :FF], acc[:, FF:]
    hid[...] = (jax.nn.silu(gate) * up).astype(BF16)
    pl.semaphore_wait(barrier, 6)

    def remote(src, dst, ss, rs, device):
        return pltpu.make_async_remote_copy(
            src_ref=src, dst_ref=dst, send_sem=ss, recv_sem=rs, device_id={"tp": device}, device_id_type=MESH
        )

    waited = set()

    def chunk(s):
        width, dims = CHUNKS[s]
        start, m = STARTS[s], len(dims)
        cols = pl.ds(start, width)
        ocols = pl.ds(pl.multiple_of(core * HALF + start, 256), width)
        pcols = pl.ds(pl.multiple_of((1 - core) * HALF + start, 256), width)
        at, sizes = [0], [NB]
        for d in dims:
            if d == "q":
                at.append(at[-1] + 2 * far + near)
                sizes.append(1)
            else:
                sizes.append(sizes[-1] // 2)
                at.append(at[-1] + bit[d] * sizes[-1])
        sends = []

        def go(j):
            return at[j] + (1 - bit[dims[j]]) * sizes[j + 1]

        def place(j):
            return 2 * NB - 2 * sizes[j + 1] if dims[j] != "q" else 28

        def rs(j):
            if dims[j] == "q":
                return [
                    remote(sbuf.at[28 + i, :, cols], rbuf.at[28 + i, :, cols], send_sem.at[s, j], recv_sem.at[s, j], device)
                    for i, (_, device) in enumerate(others)
                ]
            span = pl.ds(place(j), sizes[j + 1])
            ref = (sbuf.at[span, :, cols], rbuf.at[span, :, cols])
            return [remote(*ref, send_sem.at[s, j], recv_sem.at[s, j], peer[dims[j]])]

        def ag(j):
            span = pl.ds(at[j + 1], sizes[j + 1])
            ref = out.at[span, :, ocols]
            devices = [device for _, device in others] if dims[j] == "q" else [peer[dims[j]]]
            return [remote(ref, ref, send_sem.at[s, 4 + j], recv_sem.at[s, 4 + j], device) for device in devices]

        def core_sum():
            span = pl.ds(0, NB)
            return remote(sbuf.at[span, :, cols], rbuf.at[span, :, cols], send_core.at[s, 0], recv_core.at[s, 0], partner)

        def core_gather(i):
            span = pl.ds(at[1] if i == 0 else go(0), NB // 2)
            ref = out.at[span, :, ocols]
            return remote(ref, ref, send_core.at[s, 1 + i], recv_core.at[s, 1 + i], partner)

        def start_all(copies):
            for c in copies:
                c.start()

        def three(sem):
            ref = rbuf.at[pl.ds(28, 3), :, cols]
            pltpu.make_async_copy(ref, ref, sem).wait()

        def arrived(copies, j, sem):
            if dims[j] == "q":
                three(sem)
            else:
                copies(j)[0].wait_recv()

        def drain():
            core_sum().wait_send()
            for i in range(2):
                core_gather(i).wait_send()
            for j in range(m):
                for copies, sem in ((rs, send_sem.at[s, j]), (ag, send_sem.at[s, 4 + j])):
                    if dims[j] == "q":
                        three(sem)
                    else:
                        copies(j)[0].wait_send()

        def matmul():
            for side in (0, 1):
                for t in range(2 * (start // T) + side, 2 * ((start + width - 1) // T) + side + 1, 2):
                    if t not in waited:
                        waited.add(t)
                        down(t).wait()
                p = jnp.dot(hid[...], wd[side, :, cols], preferred_element_type=F32).reshape(NB, BLK, width)
                if side == 0:
                    sbuf[pl.ds(0, NB), :, cols] = p.astype(BF16)
                    core_sum().start()
                else:
                    own[:, :, cols] = p

        yield matmul
        for j in range(m):

            def reduce(j=j):
                if j == 0:
                    core_sum().wait_recv()
                    seen = 0
                else:
                    arrived(rs, j - 1, recv_sem.at[s, j - 1])
                    seen = place(j - 1)

                def total(first, count):
                    got = rbuf[pl.ds(seen + first - at[j], count), :, cols]
                    return own[pl.ds(first, count), :, cols] + got.astype(F32)

                if dims[j] == "q":
                    for i, (q, _) in enumerate(others):
                        sbuf[pl.ds(28 + i, 1), :, cols] = total(at[j] + q, 1).astype(BF16)
                    start_all(rs(j))
                else:
                    sbuf[pl.ds(place(j), sizes[j + 1]), :, cols] = total(go(j), sizes[j + 1]).astype(BF16)
                    start_all(rs(j))
                own[pl.ds(at[j + 1], sizes[j + 1]), :, cols] = total(at[j + 1], sizes[j + 1])

            yield reduce

        def finish():
            arrived(rs, m - 1, recv_sem.at[s, m - 1])
            count = 3 if dims[-1] == "q" else 1
            total = own[pl.ds(at[m], 1), :, cols]
            for i in range(count):
                total += rbuf[pl.ds(place(m - 1) + i, 1), :, cols].astype(F32)
            out[pl.ds(at[m], 1), :, ocols] = total.astype(BF16)
            start_all(ag(m - 1))

        yield finish
        for j in range(m - 2, -1, -1):

            def gather(j=j):
                arrived(ag, j + 1, recv_sem.at[s, 4 + j + 1])
                start_all(ag(j))
                if j == 0:
                    core_gather(0).start()

            yield gather

        def gather_core():
            arrived(ag, 0, recv_sem.at[s, 4])
            core_gather(1).start()

        yield gather_core

        def done():
            core_gather(0).wait_recv()
            core_gather(1).wait_recv()
            drain()

        yield done

    chunks = [chunk(s) for s in range(S)]
    for s in ORDER:
        task = next(chunks[s])
        with jax.named_scope(f"{task.__name__}_{s}"):
            task()


def block(x, w_gate, w_up, w_down):
    dma = pltpu.SemaphoreType.DMA
    out = pl.pallas_call(
        kernel,
        name="mlp",
        out_shape=pltpu.VMEM((NB, BLK, D), BF16),
        in_specs=[pl.BlockSpec(memory_space=pl.ANY)] * 4,
        out_specs=pl.BlockSpec(memory_space=pltpu.VMEM),
        scratch_shapes=[
            pltpu.VMEM((NS, R, 2 * FF), BF16),
            pltpu.VMEM((NS, ROWS, R), BF16),
            pltpu.VMEM((ROWS, 2 * FF), F32),
            pltpu.VMEM((ROWS, FF), BF16),
            pltpu.VMEM((2, FF, HALF), BF16),
            pltpu.VMEM((NB, BLK, HALF), F32),
            pltpu.VMEM((2 * NB, BLK, HALF), BF16),
            pltpu.VMEM((2 * NB, BLK, HALF), BF16),
            dma((3, NS)),
            dma((TILES,)),
            dma((S, 8)),
            dma((S, 8)),
            dma((S, 3)),
            dma((S, 3)),
        ],
        compiler_params=pltpu.CompilerParams(
            collective_id=0, has_side_effects=True, vmem_limit_bytes=58 * 1024 * 1024
        ),
        cost_estimate=pl.CostEstimate(flops=6 * ROWS * D * FF, bytes_accessed=6 * D * FF, transcendentals=ROWS * FF),
    )(x, w_gate, w_up, w_down)
    return out.reshape(ROWS, D)


def solution(mesh):
    return jax.shard_map(
        block,
        mesh=mesh,
        in_specs=(P("dp", None), P(None, "tp"), P(None, "tp"), P("tp", None)),
        out_specs=P("dp", None),
        check_vma=False,
    )
```

```python
import jax
import jax.numpy as jnp
from jax import lax
from jax.experimental import pallas as pl
from jax.experimental.pallas import tpu as pltpu
from jax.sharding import PartitionSpec as P

ROWS, D, FF = 128, 12288, 896
BLK = 8
NB = ROWS // BLK
R = 512
STEPS = D // R
NS = 4
HALF = D // 2
T = 1536
TILES = 2 * HALF // T
PER = TILES // NS
CHUNKS = (
    (768, "pq"), (768, "nfyX"), (768, "pq"), (256, "pq"), (768, "yxq"), (512, "nfxY"), (768, "xyq"), (768, "yxq"),
    (768, "xyq"),
)
ORDER = (
    0, 1, 0, 2, 1, 5, 2, 3, 6, 5, 4, 1, 3, 8, 6, 0, 7, 4, 2, 8, 5, 3, 6, 7, 0, 1, 4, 6, 2, 7, 8, 5, 4, 1, 3, 7, 8,
    5, 0, 6, 4, 1, 3, 8, 2, 7, 5, 3, 1, 4, 6, 8, 2, 5, 7, 4, 6, 1, 7, 8, 3, 0, 5, 2, 4, 1, 6, 4, 7, 0, 5, 6, 1, 8,
    5, 7, 8,
)
S = len(CHUNKS)
STARTS = [sum(w for w, _ in CHUNKS[:s]) for s in range(S)]
F32, BF16 = jnp.float32, jnp.bfloat16
MESH = pl.DeviceIdType.MESH


def kernel(
    x_hbm, wg_hbm, wu_hbm, wd_hbm, out,
    wbuf, xbuf, acc, hid, wd, own, sbuf, rbuf, swap,
    psem, wsem, send_rs, send_ag, send_swap, recv_sem,
):
    me = lax.axis_index("tp")
    core = lax.rem(me, 2)
    z = lax.rem(lax.div(me, 2), 4)
    y = lax.rem(lax.div(me, 8), 2)
    x = lax.div(me, 16)
    near, far = lax.rem(z, 2), lax.div(z, 2)
    partner = me + 1 - 2 * core
    bit = {"x": x, "y": y, "n": near, "f": far}
    hop = {"x": 16 * (1 - 2 * x), "y": 8 * (1 - 2 * y), "n": 2 * (1 - 2 * near), "f": 4 * (1 - 2 * far)}
    peer = {d: me + hop[d] for d in hop}

    def quad(hi, lo):
        other_hi, other_lo = 1 - bit[hi], 1 - bit[lo]
        return (
            (2 * bit[hi] + other_lo, peer[lo]),
            (2 * other_hi + bit[lo], peer[hi]),
            (2 * other_hi + other_lo, me + hop[hi] + hop[lo]),
        )

    quads = {"q": quad("f", "n"), "p": quad("x", "y")}
    place_in = {"q": 2 * far + near, "p": 2 * x + y}

    barrier = pltpu.get_barrier_semaphore()
    for device in (partner, *[device for q in quads.values() for _, device in q]):
        pl.semaphore_signal(barrier, inc=1, device_id={"tp": device}, device_id_type=MESH)

    def stream(step, slot):
        rows = pl.ds(pl.multiple_of(step * R, R), R)
        return (
            pltpu.make_async_copy(wg_hbm.at[rows, :], wbuf.at[slot, :, pl.ds(0, FF)], psem.at[0, slot]),
            pltpu.make_async_copy(wu_hbm.at[rows, :], wbuf.at[slot, :, pl.ds(FF, FF)], psem.at[0, slot]),
            pltpu.make_async_copy(x_hbm.at[:, rows], xbuf.at[slot], psem.at[1, slot]),
        )

    def down(t):
        odd = lax.rem(t, 2)
        half = odd * core + (1 - odd) * (1 - core)
        inner = lax.div(t, 2) * T
        src = wd_hbm.at[:, pl.ds(pl.multiple_of(half * HALF + inner, T), T)]
        return pltpu.make_async_copy(src, wd.at[odd, :, pl.ds(pl.multiple_of(inner, T), T)], wsem.at[t])

    def landed(ref, sem):
        pltpu.make_async_copy(ref, ref, sem).wait()

    def project(step):
        slot = lax.rem(step, NS)
        landed(wbuf.at[slot], psem.at[0, slot])
        landed(xbuf.at[slot], psem.at[1, slot])
        acc[...] += jnp.dot(xbuf[slot], wbuf[slot], preferred_element_type=F32)
        return slot

    for i in range(NS):
        for c in stream(i, i):
            c.start()
    acc[...] = jnp.zeros_like(acc)

    @pl.loop(0, STEPS - NS)
    def _(step):
        slot = project(step)
        for c in stream(step + NS, slot):
            c.start()

    @pl.loop(STEPS - NS, STEPS)
    def _(step):
        for i in range(PER):
            down(PER * (step - (STEPS - NS)) + i).start()
        project(step)

    gate, up = acc[:, :FF], acc[:, FF:]
    hid[...] = (jax.nn.silu(gate) * up).astype(BF16)
    pl.semaphore_wait(barrier, 7)

    def start(src, dst, ss, rs, device):
        pltpu.make_async_remote_copy(
            src_ref=src, dst_ref=dst, send_sem=ss, recv_sem=rs, device_id={"tp": device}, device_id_type=MESH
        ).start()

    waited = set()

    def chunk(s):
        width, dims = CHUNKS[s]
        first, m = STARTS[s], len(dims)
        cols = pl.ds(first, width)
        ocols = pl.ds(pl.multiple_of(core * HALF + first, 128), width)
        pcols = pl.ds(pl.multiple_of((1 - core) * HALF + first, 128), width)
        at, sizes = [0], [NB]
        for d in dims:
            if d in quads:
                sizes.append(sizes[-1] // 4)
                at.append(at[-1] + place_in[d] * sizes[-1])
            elif d in bit:
                sizes.append(sizes[-1] // 2)
                at.append(at[-1] + bit[d] * sizes[-1])
            else:
                sizes.append(sizes[-1])
                at.append(at[-1])
        last_gather = m - 1 if dims[-1] in quads or dims[-1] in bit else m - 2

        def targets(j):
            d, size = dims[j], sizes[j + 1]
            if d in quads:
                return [(at[j] + i * size, device) for i, device in quads[d]]
            return [(at[j] + (1 - bit[d]) * size, peer[d])]

        def held(j):
            return [2 * NB - sizes[j] + i * sizes[j + 1] for i in range(3 if dims[j] in quads else 1)]

        def arrived(j):
            if j < 0:
                landed(rbuf.at[pl.ds(0, NB), :, cols], recv_sem.at[s, 0])
            elif dims[j].isupper():
                landed(swap.at[:, :, cols], recv_sem.at[s, j + 1])
            else:
                count = len(held(j)) * sizes[j + 1]
                landed(rbuf.at[pl.ds(held(j)[0], count), :, cols], recv_sem.at[s, j + 1])

        def gathered(j):
            count = (3 if dims[j] in quads else 1) * sizes[j + 1]
            landed(rbuf.at[pl.ds(0, count), :, cols], recv_sem.at[s, j])

        def total(j, begin, count):
            value = own[pl.ds(begin, count), :, cols]
            for base in held(j) if j >= 0 else [0]:
                value += rbuf[pl.ds(base + begin - at[j + 1], count), :, cols].astype(F32)
            return value

        def give(begin, count, device, sem):
            ref = out.at[pl.ds(begin, count), :, ocols]
            start(ref, ref, send_ag.at[s], recv_sem.at[s, sem], device)

        def spread(j):
            for _, device in targets(j):
                give(at[j + 1], sizes[j + 1], device, j)
            if j == 0:
                give(at[1], sizes[1], partner, m + 1)

        def matmul():
            for side in (0, 1):
                for t in range(2 * (first // T) + side, 2 * ((first + width - 1) // T) + side + 1, 2):
                    if t not in waited:
                        waited.add(t)
                        down(t).wait()
                p = jnp.dot(hid[...], wd[side, :, cols], preferred_element_type=F32).reshape(NB, BLK, width)
                if side == 0:
                    span = pl.ds(0, NB)
                    sbuf[span, :, cols] = p.astype(BF16)
                    start(sbuf.at[span, :, cols], rbuf.at[span, :, cols], send_rs.at[s], recv_sem.at[s, 0], partner)
                else:
                    own[:, :, cols] = p

        yield matmul
        for j in range(m):

            def reduce(j=j):
                arrived(j - 1)
                size = sizes[j + 1]
                if dims[j].isupper():
                    span = pl.ds(at[j], size)
                    own[span, :, cols] = total(j - 1, at[j], size)
                    device = peer[dims[j].lower()]
                    start(own.at[span, :, cols], swap.at[:, :, cols], send_swap.at[s], recv_sem.at[s, j + 1], device)
                    return
                for base, (begin, device) in zip(held(j), targets(j), strict=True):
                    span = pl.ds(base, size)
                    sbuf[span, :, cols] = total(j - 1, begin, size).astype(BF16)
                    start(sbuf.at[span, :, cols], rbuf.at[span, :, cols], send_rs.at[s], recv_sem.at[s, j + 1], device)
                own[pl.ds(at[j + 1], size), :, cols] = total(j - 1, at[j + 1], size)

            yield reduce

        def finish():
            arrived(m - 1)
            span = pl.ds(at[m], sizes[m])
            if dims[-1].isupper():
                value = own[span, :, cols] + swap[:, :, cols]
            else:
                value = total(m - 1, at[m], sizes[m])
            out[span, :, ocols] = value.astype(BF16)
            spread(last_gather)

        yield finish
        for j in range(last_gather - 1, -1, -1):

            def gather(j=j):
                gathered(j + 1)
                spread(j)

            yield gather

        def gather_core():
            gathered(0)
            for begin, _ in targets(0):
                give(begin, sizes[1], partner, m + 1)

        yield gather_core

        def done():
            landed(out.at[:, :, pcols], recv_sem.at[s, m + 1])

        yield done

    chunks = [chunk(s) for s in range(S)]
    for s in ORDER:
        task = next(chunks[s])
        with jax.named_scope(f"{task.__name__}_{s}"):
            task()
    for s, (width, dims) in enumerate(CHUNKS):
        cols = pl.ds(STARTS[s], width)
        swaps = dims[-1].isupper()
        sent = sbuf.at[pl.ds(0, 2 * NB - (2 if swaps else 1)), :, cols]
        landed(sent, send_rs.at[s])
        landed(sent, send_ag.at[s])
        if swaps:
            landed(swap.at[:, :, cols], send_swap.at[s])


def block(x, w_gate, w_up, w_down):
    dma = pltpu.SemaphoreType.DMA
    out = pl.pallas_call(
        kernel,
        name="mlp",
        out_shape=pltpu.VMEM((NB, BLK, D), BF16),
        in_specs=[pl.BlockSpec(memory_space=pl.ANY)] * 4,
        out_specs=pl.BlockSpec(memory_space=pltpu.VMEM),
        scratch_shapes=[
            pltpu.VMEM((NS, R, 2 * FF), BF16),
            pltpu.VMEM((NS, ROWS, R), BF16),
            pltpu.VMEM((ROWS, 2 * FF), F32),
            pltpu.VMEM((ROWS, FF), BF16),
            pltpu.VMEM((2, FF, HALF), BF16),
            pltpu.VMEM((NB, BLK, HALF), F32),
            pltpu.VMEM((2 * NB, BLK, HALF), BF16),
            pltpu.VMEM((2 * NB, BLK, HALF), BF16),
            pltpu.VMEM((2, BLK, HALF), F32),
            dma((2, NS)),
            dma((TILES,)),
            dma((S,)),
            dma((S,)),
            dma((S,)),
            dma((S, 2 + max(len(dims) for _, dims in CHUNKS))),
        ],
        compiler_params=pltpu.CompilerParams(
            collective_id=0, has_side_effects=True, vmem_limit_bytes=50 * 1024 * 1024
        ),
        cost_estimate=pl.CostEstimate(flops=6 * ROWS * D * FF, bytes_accessed=6 * D * FF, transcendentals=ROWS * FF),
    )(x, w_gate, w_up, w_down)
    return out.reshape(ROWS, D)


def solution(mesh):
    return jax.shard_map(
        block,
        mesh=mesh,
        in_specs=(P("dp", None), P(None, "tp"), P(None, "tp"), P("tp", None)),
        out_specs=P("dp", None),
        check_vma=False,
    )
```
